512 devices in a mesh: groups: 2 (over y), seq: 16 (over z), head: 8 (over x), sub: 2 (over core).
Axes of the slice: x: 8, y: 2, z: 16, core: 2. Of those that a mesh axis runs over, the one named last changes fastest.
The devices are a block of a 8x8x16 slice.
Arguments:
- queries: bfloat16 [32768, 4096], P(('groups', 'seq'), 'head'), parts along dimension 0, may hold values from -48 to 48
- keys: bfloat16 [32768, 1024], P(('groups', 'seq', 'sub'), 'head'), parts along dimension 0, may hold values from -18 to 18
- values: bfloat16 [32768, 1024], P(('groups', 'seq', 'sub'), 'head'), parts along dimension 0, may hold values from -6 to 6
- doc_lengths: int32 [64], P('groups'), parts along dimension 0, may hold values from 1 to 2048, 16384 in all
Outputs:
- attended: bfloat16 [32768, 4096], P(('groups', 'seq'), 'head'), parts along dimension 0
The draws below stay inside these ranges and needn't reach their ends.
There are 2 independent parts, one for each index of `groups`. The reference program is written for one: setup_inputs(seed, part) draws one part's arguments, and reference() takes and returns one part's arrays. A program takes and returns all parts, laid end to end along the dimension named above; each array names one. Nothing has to cross between parts.
Inputs may be any that keep to these rules, and one draw needn't show every extreme that they name: `doc_lengths`: the 32 lengths sum to 16384; one of them is exactly 2048.
All inputs are finite; a program needn't handle non-finite values.
Results may differ from the reference program's by a relative error of at most 0.0036.
Values may be sent and summed in bfloat16 or wider, within the bound.
A program may use at most 64 MiB of HBM per device.

```python
import math
import jax
import jax.numpy as jnp
import numpy as np
from jax import lax

QH = 32
KVH = 8
DH = 128
TOK_DEV = 1024
SEQLEN = 16384
NDOCS = 32
MAXDOC = 2048
N_SEQ = 16


def shared_rows(key):
    width = KVH * DH
    drawn = jnp.clip(jax.random.normal(jax.random.fold_in(key, 11), (SEQLEN, width), jnp.float32), -6.0, 6.0)
    return drawn


def draw_keys(key, part):
    drawn = shared_rows(key)
    return drawn.astype(jnp.bfloat16)


def draw_queries(key, part):
    base_rows = jnp.clip(jax.random.normal(jax.random.fold_in(key, 19), (SEQLEN, QH * DH), jnp.float32), -6.0, 6.0)
    return base_rows.astype(jnp.bfloat16)


def levels(rng, extent, pieces, low, high):
    gain = 1.0
    for axis_at, parts in pieces:
        heights = jax.random.uniform(jax.random.fold_in(jax.random.fold_in(rng, 6), axis_at), (parts,), jnp.float32, low / len(pieces), high / len(pieces))
        gain = gain * jnp.repeat(jnp.exp(heights), extent[axis_at] // parts).reshape((-1,) + (1,) * (len(extent) - 1 - axis_at))
    return gain


def profile(number_of, total, reach, skew):
    loads = [(1 << 20) // math.isqrt(rank ** skew) + 1 for rank in range(2, number_of + 1)]
    spare, counts = total - reach - (number_of - 1), [1] * (number_of - 1)
    while spare > 0:
        candidates = [i for i in range(number_of - 1) if counts[i] < reach]
        mass, budget = sum([loads[i] for i in candidates]), spare
        for i in candidates:
            more = min(reach - counts[i], max(1, budget * loads[i] // mass), spare)
            counts[i] = counts[i] + more
            spare = spare - more
    return np.array([reach] + counts)


def ragged(key, number_of, total, reach, slope):
    if number_of == 2:
        one = jax.random.randint(key, (), max(1, total - reach), min(reach, total - 1) + 1)
        return jnp.stack([one, total - one])
    tallies = jnp.asarray(profile(number_of, total, reach, slope), jnp.int32)
    couples = (number_of - 1) // 2
    source_of, taker = tallies[1:1 + 2 * couples:2], tallies[2:2 + 2 * couples:2]
    margin = jnp.minimum(source_of - 1, reach - taker)
    moved = jax.random.randint(jax.random.fold_in(key, 1), (couples,), 0, 1 << 20) % (margin + 1)
    tallies = tallies.at[1:1 + 2 * couples:2].set(source_of - moved).at[2:2 + 2 * couples:2].set(taker + moved)
    return tallies[jax.random.permutation(jax.random.fold_in(key, 2), number_of)]


def centred(own_key, extent, scale, bound, split=(), held_as=jnp.bfloat16):
    level = levels(own_key, extent, split, -0.22, 0.18) if split else 1.0
    array = jax.random.normal(own_key, extent, jnp.float32) * scale * level
    return jnp.minimum(jnp.maximum(array, -bound), bound).astype(held_as)


def setup_inputs(seed: int = 0, part: int = 0) -> dict:
    key_of = jax.random.split(jax.random.key(seed), 5)
    part_keys = jax.random.split(jax.random.fold_in(key_of[4], part), 5)
    queries = draw_queries(jax.random.fold_in(jax.random.fold_in(key_of[4], part), 71), part)
    keys = draw_keys(jax.random.fold_in(jax.random.fold_in(key_of[4], part), 71), part)
    values = centred(part_keys[2], (SEQLEN, KVH * DH), 1.0, 6.0, ((0, 32), (1, 8)))
    doc_lengths = ragged(part_keys[3], NDOCS, SEQLEN, MAXDOC, 2).astype(jnp.int32)
    return {"queries": queries, "keys": keys, "values": values, "doc_lengths": doc_lengths}


def reference(queries, keys, values, doc_lengths):
    per_group = QH // KVH
    window = MAXDOC + TOK_DEV
    starts = jnp.cumsum(doc_lengths) - doc_lengths
    positions = jnp.arange(SEQLEN, dtype=jnp.int32)
    doc_of = lax.optimization_barrier(jnp.sum((starts[None, :] <= positions[:, None]).astype(jnp.int32), axis=1)) - 1
    padded_keys = jnp.concatenate([jnp.zeros((MAXDOC, KVH * DH), keys.dtype), keys], axis=0)
    padded_values = jnp.concatenate([jnp.zeros((MAXDOC, KVH * DH), values.dtype), values], axis=0)
    padded_docs = jnp.concatenate([jnp.full((MAXDOC,), -1, jnp.int32), doc_of.astype(jnp.int32)], axis=0)
    scaling = 1.0 / math.sqrt(DH)

    def one_block(number):
        first = (number * TOK_DEV).astype(jnp.int32)
        query_rows = lax.dynamic_slice_in_dim(queries, first, TOK_DEV, 0).astype(jnp.float32)
        query_rows = query_rows.reshape(TOK_DEV, KVH, per_group, DH)
        key_rows = lax.dynamic_slice_in_dim(padded_keys, first, window, 0).astype(jnp.float32)
        value_rows = lax.dynamic_slice_in_dim(padded_values, first, window, 0).astype(jnp.float32)
        query_pos = first + jnp.arange(TOK_DEV, dtype=jnp.int32)
        query_doc = lax.dynamic_slice_in_dim(doc_of.astype(jnp.int32), first, TOK_DEV, 0)
        key_pos = first - MAXDOC + jnp.arange(window, dtype=jnp.int32)
        key_doc = lax.dynamic_slice_in_dim(padded_docs, first, window, 0)
        allowed = (key_pos[None, :] <= query_pos[:, None]) & (key_doc[None, :] == query_doc[:, None])
        outputs = []
        for head_pair in range(KVH):
            head_keys = key_rows[:, head_pair * DH:(head_pair + 1) * DH]
            head_values = value_rows[:, head_pair * DH:(head_pair + 1) * DH]
            scores = jnp.einsum('qgd,kd->qgk', query_rows[:, head_pair], head_keys) * scaling
            scores = jnp.where(allowed[:, None, :], scores, -jnp.inf)
            highest = lax.optimization_barrier(jnp.max(scores, axis=-1))
            expo = jnp.exp(scores - highest[..., None])
            denom = lax.optimization_barrier(jnp.sum(expo, axis=-1))
            weight = lax.optimization_barrier(expo.astype(jnp.bfloat16)).astype(jnp.float32)
            summed = jnp.einsum('qgk,kd->qgd', weight, head_values)
            outputs.append(summed / denom[..., None])
        stacked = jnp.stack(outputs, axis=1)
        return stacked.reshape(TOK_DEV, QH * DH).astype(jnp.bfloat16)
    result = lax.map(one_block, jnp.arange(N_SEQ, dtype=jnp.int32))
    return result.reshape(SEQLEN, QH * DH)
```

```python
import math

import jax
import jax.numpy as jnp
from jax import lax
from jax.experimental import pallas as pl
from jax.experimental.pallas import tpu as pltpu
from jax.sharding import PartitionSpec as P

DH = 128
PARTS = 4
MASKED = -1e30
FAR = 1 << 29
LOG2E = 1.4426950408889634
MESH = pl.DeviceIdType.MESH
NT = (((1,), (1,)), ((), ()))
NN = (((1,), (0,)), ((), ()))


def matmul(a, b, dims):
    return lax.dot_general(a, b, dims, preferred_element_type=jnp.float32)


def twice(x):
    return jnp.concatenate([x, x], axis=1)


def document_table(lens, shape):
    lane = lax.broadcasted_iota(jnp.int32, shape, 1)
    first = jnp.full(shape, FAR, jnp.int32)
    end = jnp.full(shape, FAR, jnp.int32)
    count = lens.shape[0]
    total = jnp.int32(0)
    for d in range(count):
        here = lane == d
        first = jnp.where(here, total, first)
        total = total + lens[d]
        end = jnp.where(here, total, end)
    before = lane == count
    return jnp.where(before, -FAR, first), jnp.where(before, 0, end)


def body(q_hbm, k_hbm, v_hbm, lens, out, qv, kb, vb, kx, qx, acc, top, ob,
         load_sem, near_sem, far_sem, own_sem, near_peer_sem, far_peer_sem, out_sem):
    z, c = lax.axis_index("seq"), lax.axis_index("sub")
    count = lax.axis_size("seq")
    after, ahead = lax.rem(z + 1, count), lax.rem(z + count - 1, count)
    half = k_hbm.shape[0]
    rows = 2 * half
    part = half // PARTS
    width = qv.shape[1]
    heads = width // DH
    scale = LOG2E / math.sqrt(DH)

    loads = [
        pltpu.make_async_copy(k_hbm, kb.at[0, pl.ds(pl.multiple_of(c * half, half), half)], load_sem.at[0]),
        pltpu.make_async_copy(v_hbm, vb.at[0, pl.ds(pl.multiple_of(c * half, half), half)], load_sem.at[1]),
        pltpu.make_async_copy(q_hbm.at[:, pl.ds(pl.multiple_of(c * width, width), width)], qv, load_sem.at[2]),
    ]
    for copy in loads:
        copy.start()

    barrier = pltpu.get_barrier_semaphore()
    pl.semaphore_signal(barrier, inc=1, device_id={"seq": ahead}, device_id_type=MESH)
    pl.semaphore_signal(barrier, inc=1, device_id={"sub": 1 - c}, device_id_type=MESH)
    pl.semaphore_wait(barrier, 2)

    def block_copy(buf, source, target, start, size, sems, index, device):
        return pltpu.make_async_remote_copy(
            src_ref=buf.at[source, pl.ds(start, size)],
            dst_ref=buf.at[target, pl.ds(start, size)],
            send_sem=sems.at[(0, *index)],
            recv_sem=sems.at[(1, *index)],
            device_id=device,
            device_id_type=MESH,
        )

    def pair(source, target, start, size, sems, n, device):
        return [
            block_copy(kb, source, target, start, size, sems, (n, 0), device),
            block_copy(vb, source, target, start, size, sems, (n, 1), device),
        ]

    def part_start(n):
        return pl.multiple_of(c * half + (PARTS - 1 - n) * part, part)

    onward, peer = {"seq": after}, {"sub": 1 - c}
    near = [pair(0, 1, part_start(n), part, near_sem, n, onward) for n in range(PARTS)]
    far = [pair(1, 2, part_start(n), part, far_sem, n, onward) for n in range(PARTS)]
    own_peer = pair(0, 0, pl.multiple_of(c * half, half), half, own_sem, 0, peer)
    near_peer = [pair(1, 1, part_start(n), part, near_peer_sem, n, peer) for n in range(PARTS)]
    far_peer = [pair(2, 2, part_start(n), part, far_peer_sem, n, peer) for n in range(PARTS)]

    loads[0].wait()
    near[0][0].start()
    loads[1].wait()
    near[0][1].start()
    for copy in own_peer:
        copy.start()
    for copies in near[1:]:
        for copy in copies:
            copy.start()

    first, end = document_table(lens, (1, 128))

    def in_document(position):
        return (position >= first) & (position < end)

    row = lax.broadcasted_iota(jnp.int32, (part, 128), 0)
    for tile in range(rows // part):
        at = pl.ds(tile * part, part)
        member = in_document(row + (z * rows + tile * part))
        kx[0, at] = jnp.where(member, 1.0, 0.0).astype(jnp.bfloat16)
        qx[at] = jnp.where(member, 0.0, MASKED).astype(jnp.bfloat16)

    ones = jnp.ones((part, 128), jnp.bfloat16)

    def keys_of(block, starts, size):
        return jnp.concatenate(
            [jnp.concatenate([kb[block, pl.ds(s, size)], kx[block, pl.ds(s, size)]], axis=1) for s in starts], axis=0
        )

    def values_of(block, starts, size):
        return jnp.concatenate(
            [jnp.concatenate([vb[block, pl.ds(s, size)], jnp.ones((size, 128), jnp.bfloat16)], axis=1) for s in starts],
            axis=0,
        )

    def queries_of(h, start, size):
        return jnp.concatenate([qv[pl.ds(start, size), pl.ds(h * DH, DH)], qx[pl.ds(start, size)]], axis=1)

    def row_top(scores):
        best = scores[:, :128]
        for n in range(1, scores.shape[1] // 128):
            best = jnp.maximum(best, scores[:, n * 128 : (n + 1) * 128])
        return jnp.max(best, axis=1, keepdims=True)

    def expo(scores, highest):
        return jnp.concatenate(
            [
                jnp.exp2((scores[:, n * 128 : (n + 1) * 128] - highest) * scale).astype(jnp.bfloat16)
                for n in range(scores.shape[1] // 128)
            ],
            axis=1,
        )

    loads[2].wait()
    for copy in own_peer:
        copy.wait_recv()

    causal = lax.broadcasted_iota(jnp.int32, (part, part), 1) <= lax.broadcasted_iota(jnp.int32, (part, part), 0)
    for tile in range(rows // part):
        span = (tile + 1) * part
        these_keys, these_values = keys_of(0, [0], span), values_of(0, [0], span)
        for h in range(heads):
            scores = matmul(queries_of(h, tile * part, part), these_keys, NT)
            last = jnp.where(causal, scores[:, span - part :], MASKED)
            scores = jnp.concatenate([scores[:, : span - part], last], axis=1) if tile else last
            highest = jnp.broadcast_to(row_top(scores), (part, 128))
            top[h, pl.ds(tile * part, part)] = highest
            acc[h, pl.ds(tile * part, part)] = matmul(expo(scores, highest), these_values, NN)

    for block in (1, 2):
        for tile in range(rows // part):
            at = pl.ds(tile * part, part)
            member = in_document(row + ((z - block) * rows + tile * part))
            kx[block, at] = jnp.where(member, 1.0, 0.0).astype(jnp.bfloat16)

    def update(h, start, size, these_keys, these_values):
        at = pl.ds(start, size)
        scores = matmul(queries_of(h, start, size), these_keys, NT)
        before = top[h, at]
        highest = jnp.maximum(before, row_top(scores))
        fade = jnp.exp2((before - highest) * scale)
        top[h, at] = highest
        acc[h, at] = acc[h, at] * twice(fade) + matmul(expo(scores, highest), these_values, NN)

    out_copies = []

    def finish(start, size):
        at = pl.ds(start, size)
        for h in range(heads):
            total = acc[h, at]
            ob[at, pl.ds(h * DH, DH)] = (total[:, :DH] / total[:, DH:]).astype(jnp.bfloat16)
        n = len(out_copies)
        place = out.at[at, pl.ds(pl.multiple_of(c * width, width), width)]
        here = pltpu.make_async_copy(ob.at[at], place, out_sem.at[2, n])
        there = pltpu.make_async_remote_copy(
            src_ref=ob.at[at],
            dst_ref=place,
            send_sem=out_sem.at[0, n],
            recv_sem=out_sem.at[1, n],
            device_id=peer,
            device_id_type=MESH,
        )
        there.start()
        here.start()
        out_copies.append((here, there))

    def arrive(g):
        copies = near[g] if g < PARTS else far[g - PARTS]
        relays = near_peer[g] if g < PARTS else far_peer[g - PARTS]
        forwards = far[g] if g < PARTS else [None, None]
        for copy, relay, forward in zip(copies, relays, forwards):
            copy.wait_recv()
            relay.start()
            if forward is not None:
                forward.start()

    arrive(0)
    for g in range(2 * PARTS):
        if g + 1 < 2 * PARTS:
            arrive(g + 1)
        n = g % PARTS
        block = 1 if g < PARTS else 2
        for copy in near_peer[n] if g < PARTS else far_peer[n]:
            copy.wait_recv()
        low = (PARTS - 1 - n) * part
        both = [low, half + low]
        if g < PARTS:
            these_keys, these_values = keys_of(1, both, part), values_of(1, both, part)
            for h in range(heads):
                for start in range(0, rows, half):
                    update(h, start, half, these_keys, these_values)
        else:
            these_keys, these_values = keys_of(2, both, part), values_of(2, both, part)
            upper_keys, upper_values = keys_of(2, both[1:], part), values_of(2, both[1:], part)
            for h in range(heads):
                update(h, 0, low + part, these_keys, these_values)
                update(h, low + part, half, upper_keys, upper_values)
            if n < PARTS - 1:
                finish(half + low, part)
            else:
                finish(0, half + part)

    for copies in [*near, *far, own_peer, *near_peer, *far_peer]:
        for copy in copies:
            copy.wait_send()
    for here, there in out_copies:
        here.wait()
        there.wait()


def shards(queries, keys, values, doc_lengths):
    rows, width = queries.shape
    half = keys.shape[0]
    mine = width // 2
    heads = mine // DH
    whole = pl.BlockSpec(memory_space=pl.ANY)
    return pl.pallas_call(
        body,
        out_shape=jax.ShapeDtypeStruct(queries.shape, queries.dtype),
        in_specs=[whole, whole, whole, pl.BlockSpec(memory_space=pltpu.SMEM)],
        out_specs=whole,
        scratch_shapes=[
            pltpu.VMEM((rows, mine), jnp.bfloat16),
            pltpu.VMEM((3, rows, DH), jnp.bfloat16),
            pltpu.VMEM((3, rows, DH), jnp.bfloat16),
            pltpu.VMEM((3, rows, 128), jnp.bfloat16),
            pltpu.VMEM((rows, 128), jnp.bfloat16),
            pltpu.VMEM((heads, rows, 2 * DH), jnp.float32),
            pltpu.VMEM((heads, rows, 128), jnp.float32),
            pltpu.VMEM((rows, mine), jnp.bfloat16),
            pltpu.SemaphoreType.DMA((3,)),
            pltpu.SemaphoreType.DMA((2, PARTS, 2)),
            pltpu.SemaphoreType.DMA((2, PARTS, 2)),
            pltpu.SemaphoreType.DMA((2, 1, 2)),
            pltpu.SemaphoreType.DMA((2, PARTS, 2)),
            pltpu.SemaphoreType.DMA((2, PARTS, 2)),
            pltpu.SemaphoreType.DMA((3, PARTS)),
        ],
        compiler_params=pltpu.CompilerParams(collective_id=0, has_side_effects=True),
        name="packed_attention",
    )(queries, keys, values, doc_lengths)


def solution(mesh):
    placed = (
        P(("groups", "seq"), "head"),
        P(("groups", "seq", "sub"), "head"),
        P(("groups", "seq", "sub"), "head"),
        P("groups"),
    )
    return jax.shard_map(
        shards, mesh=mesh, in_specs=placed, out_specs=P(("groups", "seq"), "head"), check_vma=False
    )
```
